8 devices in a mesh: dp: 2 (over z, y), cp: 4 (over x, core).
Axes of the slice: x: 2, y: 2, z: 1, core: 2. Of those that a mesh axis runs over, the one named last changes fastest.
Arguments:
- hidden_states: bfloat16 [2, 8192, 896], P('dp', 'cp')
- norm_gain: float32 [896], replicated
- w_gate: bfloat16 [896, 4864], replicated
- w_up: bfloat16 [896, 4864], replicated
- w_down: bfloat16 [4864, 896], replicated
- final_gain: float32 [896], replicated
- w_value: float32 [896], replicated
- b_value: float32 [], replicated
- rewards: float32 [2, 8192], P('dp', 'cp')
- mask: int32 [2, 8192], P('dp', 'cp')
Outputs:
- output 1: float32 [2, 8192], P('dp', 'cp')
- output 2: float32 [2, 8192], P('dp', 'cp')
- output 3: float32 [2, 8192], P('dp', 'cp')
All inputs are finite; a program needn't handle non-finite values.
Results may differ from the reference program's by a relative error of at most 0.001.
Values sent between devices are 32-bit elements.
A program may use at most 1 GiB of HBM per device.

```python
import jax
import jax.numpy as jnp
from jax import lax

ROW_COUNT = 2
SEQ_LEN = 8192
MODEL_DIM = 896
FFN_DIM = 4864
NORM_EPS = 1e-6
WHITEN_EPS = 1e-8
DISCOUNT = 1.0
GAE_LAMBDA = 0.995


def draw_mask(start_key, end_key):
    starts = jax.random.randint(start_key, (ROW_COUNT,), 0, SEQ_LEN // 2)
    ends = starts + jax.random.randint(end_key, (ROW_COUNT,), 0, SEQ_LEN - starts)
    positions = jnp.arange(SEQ_LEN)[None, :]
    inside = (positions >= starts[:, None]) & (positions <= ends[:, None])
    return inside.astype(jnp.int32), ends


def setup_inputs(seed: int = 0) -> dict:
    keys = jax.random.split(jax.random.key(seed), 12)
    hidden_states = jax.random.normal(keys[0], (ROW_COUNT, SEQ_LEN, MODEL_DIM), jnp.float32).astype(jnp.bfloat16)
    norm_gain = 1.0 + 0.3 * jax.random.normal(keys[1], (MODEL_DIM,), jnp.float32)
    w_gate = (jax.random.normal(keys[2], (MODEL_DIM, FFN_DIM), jnp.float32) * MODEL_DIM ** -0.5).astype(jnp.bfloat16)
    w_up = (jax.random.normal(keys[3], (MODEL_DIM, FFN_DIM), jnp.float32) * MODEL_DIM ** -0.5).astype(jnp.bfloat16)
    w_down = (jax.random.normal(keys[4], (FFN_DIM, MODEL_DIM), jnp.float32) * FFN_DIM ** -0.5).astype(jnp.bfloat16)
    final_gain = 1.0 + 0.3 * jax.random.normal(keys[5], (MODEL_DIM,), jnp.float32)
    w_value = jax.random.normal(keys[6], (MODEL_DIM,), jnp.float32) * MODEL_DIM ** -0.5
    b_value = jax.random.uniform(keys[7], (), jnp.float32, 0.5, 1.0)
    mask, ends = draw_mask(keys[8], keys[9])
    shaping = 0.05 * jax.random.normal(keys[10], (ROW_COUNT, SEQ_LEN), jnp.float32)
    score = 2.0 * jax.random.normal(keys[11], (ROW_COUNT,), jnp.float32)
    at_end = jnp.arange(SEQ_LEN)[None, :] == ends[:, None]
    rewards = shaping + jnp.where(at_end, score[:, None], 0.0)
    return dict(hidden_states=hidden_states, norm_gain=norm_gain, w_gate=w_gate, w_up=w_up, w_down=w_down, final_gain=final_gain, w_value=w_value, b_value=b_value, rewards=rewards, mask=mask)


def reference(hidden_states, norm_gain, w_gate, w_up, w_down, final_gain, w_value, b_value, rewards, mask):
    head_vec = final_gain * w_value

    def row_value(x_row):
        x_f32 = x_row.astype(jnp.float32)
        normed = (x_f32 * lax.rsqrt(jnp.mean(x_f32 * x_f32, axis=-1, keepdims=True) + NORM_EPS) * norm_gain).astype(jnp.bfloat16)
        gate = jnp.dot(normed, w_gate, preferred_element_type=jnp.float32)
        up_val = jnp.dot(normed, w_up, preferred_element_type=jnp.float32)
        hidden = (jax.nn.silu(gate) * up_val).astype(jnp.bfloat16)
        resid = x_f32 + jnp.dot(hidden, w_down, preferred_element_type=jnp.float32)
        resid_n = resid * lax.rsqrt(jnp.mean(resid * resid, axis=-1, keepdims=True) + NORM_EPS)
        return jnp.sum(resid_n * head_vec, axis=-1) + b_value

    mask_f = mask.astype(jnp.float32)
    values = mask_f * lax.map(row_value, hidden_states)
    rew_masked = mask_f * rewards
    next_vals = jnp.concatenate([values[:, 1:], jnp.zeros_like(values[:, :1])], axis=1)
    delta = rew_masked + DISCOUNT * next_vals - values

    def back_step(carry, delta_col):
        adv_col = delta_col + DISCOUNT * GAE_LAMBDA * carry
        return adv_col, adv_col

    _, adv_cols = lax.scan(back_step, jnp.zeros_like(delta[:, 0]), delta.T, reverse=True)
    advantage = adv_cols.T
    count = jnp.sum(mask_f)
    mean_adv = jnp.sum(mask_f * advantage) / count
    var_adv = jnp.sum(mask_f * advantage * advantage) / count - mean_adv * mean_adv
    white = mask_f * (advantage - mean_adv) * lax.rsqrt(var_adv + WHITEN_EPS)
    return values, mask_f * (advantage + values), white
```

```python
import math
import functools
import jax
import jax.numpy as jnp
from jax import lax
from jax.sharding import PartitionSpec as P
from jax.experimental import pallas as pl
from jax.experimental.pallas import tpu as pltpu

NORM_EPS = 1e-6
WHITEN_EPS = 1e-8
DISCOUNT = 1.0
GAE_LAMBDA = 0.995
LOG_DECAY = math.log(DISCOUNT * GAE_LAMBDA)
DECAY = DISCOUNT * GAE_LAMBDA
LANES = 128
BLOCK = 256
COLS = 512


def chunks(total, step):
    return [(start, min(step, total - start)) for start in range(0, total, step)]


def mlp_kernel(mask_ref, gain_ref, final_ref, wval_ref, bias_ref, x_hbm, wg_hbm, wu_hbm, wd_hbm, out_ref,
               x_v, n_v, u_v, wg_v, wu_v, wd_v, val_v, x_sem, w_sem, d_sem):
    seq, dim = x_hbm.shape
    ffn = wg_v.shape[1]
    cols = chunks(ffn, COLS)

    def up_copies(i):
        c, w = cols[i]
        return (pltpu.make_async_copy(wg_hbm.at[:, pl.ds(c, w)], wg_v.at[:, pl.ds(c, w)], w_sem.at[0, i]),
                pltpu.make_async_copy(wu_hbm.at[:, pl.ds(c, w)], wu_v.at[:, pl.ds(c, w)], w_sem.at[1, i]))

    down_copy = pltpu.make_async_copy(wd_hbm, wd_v, d_sem)

    mask = mask_ref[...]
    rows = lax.broadcasted_iota(jnp.int32, mask.shape, 0)
    lanes = lax.broadcasted_iota(jnp.int32, mask.shape, 1)
    pos = rows * LANES + lanes
    first = jnp.min(jnp.where(mask > 0, pos, seq))
    last = jnp.max(jnp.where(mask > 0, pos, -1))
    first = (first // 16) * 16
    count = jnp.where(last >= 0, (last - first) // BLOCK + 1, 0)

    def start_of(i):
        return pl.multiple_of(jnp.minimum(first + i * BLOCK, seq - BLOCK), 16)

    def x_copy(i):
        slot = lax.rem(i, 2)
        return pltpu.make_async_copy(x_hbm.at[pl.ds(start_of(i), BLOCK), :], x_v.at[slot], x_sem.at[slot])

    def block(i, waits):
        slot = lax.rem(i, 2)
        x_copy(i).wait()

        @pl.when(i + 1 < count)
        def _():
            x_copy(i + 1).start()

        xf = x_v[slot].astype(jnp.float32)
        scale = lax.rsqrt(jnp.mean(xf * xf, axis=-1, keepdims=True) + NORM_EPS)
        n_v[...] = (xf * scale * gain_ref[...]).astype(jnp.bfloat16)
        for j, (c, w) in enumerate(cols):
            if waits:
                for copy in up_copies(j):
                    copy.wait()
            gate = jnp.dot(n_v[...], wg_v[:, c:c + w], preferred_element_type=jnp.float32)
            up = jnp.dot(n_v[...], wu_v[:, c:c + w], preferred_element_type=jnp.float32)
            u_v[:, c:c + w] = (jax.nn.silu(gate) * up).astype(jnp.bfloat16)
        if waits:
            down_copy.wait()
        h = x_v[slot].astype(jnp.float32) + jnp.dot(u_v[...], wd_v[...], preferred_element_type=jnp.float32)
        square = jnp.mean(h * h, axis=-1, keepdims=True)
        proj = jnp.sum(h * (final_ref[...] * wval_ref[...]), axis=-1, keepdims=True)
        val = proj * lax.rsqrt(square + NORM_EPS) + bias_ref[0]
        val_v[pl.ds(start_of(i), BLOCK), :] = jnp.broadcast_to(val, (BLOCK, LANES))

    @pl.when(count > 0)
    def _():
        x_copy(0).start()
        for i in range(len(cols)):
            for copy in up_copies(i):
                copy.start()
        down_copy.start()
        block(0, True)

        @pl.loop(1, count)
        def _(i):
            block(i, False)

    eye = lax.broadcasted_iota(jnp.int32, (LANES, LANES), 0) == lax.broadcasted_iota(jnp.int32, (LANES, LANES), 1)
    for r in range(seq // LANES):
        row = jnp.sum(jnp.where(eye, val_v[r * LANES:(r + 1) * LANES, :], 0.0), axis=0, keepdims=True)
        out_ref[r:r + 1, :] = jnp.where(mask_ref[r:r + 1, :] > 0, row, 0.0)


def mlp_values(mask2, norm_gain, final_gain, w_value, b_value, x, w_gate, w_up, w_down):
    seq, dim = x.shape
    ffn = w_gate.shape[1]
    vmem = pl.BlockSpec(memory_space=pltpu.VMEM)
    hbm = pl.BlockSpec(memory_space=pl.ANY)
    n_cols = len(chunks(ffn, COLS))
    return pl.pallas_call(
        mlp_kernel,
        out_shape=jax.ShapeDtypeStruct((seq // LANES, LANES), jnp.float32),
        in_specs=[vmem, vmem, vmem, vmem, pl.BlockSpec(memory_space=pltpu.SMEM), hbm, hbm, hbm, hbm],
        out_specs=vmem,
        scratch_shapes=[
            pltpu.VMEM((2, BLOCK, dim), jnp.bfloat16),
            pltpu.VMEM((BLOCK, dim), jnp.bfloat16),
            pltpu.VMEM((BLOCK, ffn), jnp.bfloat16),
            pltpu.VMEM((dim, ffn), jnp.bfloat16),
            pltpu.VMEM((dim, ffn), jnp.bfloat16),
            pltpu.VMEM((ffn, dim), jnp.bfloat16),
            pltpu.VMEM((seq, LANES), jnp.float32),
            pltpu.SemaphoreType.DMA((2,)),
            pltpu.SemaphoreType.DMA((2, n_cols)),
            pltpu.SemaphoreType.DMA,
        ],
        compiler_params=pltpu.CompilerParams(vmem_limit_bytes=60 * 1024 * 1024),
        cost_estimate=pl.CostEstimate(flops=6 * seq * dim * ffn, bytes_accessed=3 * 2 * dim * ffn, transcendentals=seq * ffn),
        name="critic_mlp",
    )(mask2, norm_gain[None, :], final_gain[None, :], w_value[None, :], b_value[None], x, w_gate, w_up, w_down)


def tail_kernel(dp_size, cp_size, val_ref, rew_ref, mask_ref, ret_ref, white_ref, send, recv, send_sem, recv_sem):
    n_dev = dp_size * cp_size
    n_rows = val_ref.shape[0]
    seq = n_rows * LANES
    me = lax.axis_index('dp') * cp_size + lax.axis_index('cp')
    barrier = pltpu.get_barrier_semaphore()

    def peer(k):
        other = lax.rem(me + k, n_dev)
        return {'dp': other // cp_size, 'cp': lax.rem(other, cp_size)}

    for k in range(1, n_dev):
        pl.semaphore_signal(barrier, inc=1, device_id=peer(k), device_id_type=pl.DeviceIdType.MESH)

    val = val_ref[...]
    mask = mask_ref[...].astype(jnp.float32)
    rows = lax.broadcasted_iota(jnp.int32, val.shape, 0)
    lanes = lax.broadcasted_iota(jnp.int32, val.shape, 1)
    pos = rows * LANES + lanes

    def up_rows(a, k):
        return jnp.where(rows < n_rows - k, pltpu.roll(a, n_rows - k, 0), 0.0)

    shifted = pltpu.roll(val, LANES - 1, 1)
    next_val = jnp.where(lanes < LANES - 1, shifted, up_rows(shifted, 1))
    adv = mask * rew_ref[...] + DISCOUNT * next_val - val
    k = 1
    while k < LANES:
        adv = adv + DECAY ** k * jnp.where(lanes < LANES - k, pltpu.roll(adv, LANES - k, 1), 0.0)
        k *= 2
    head = jnp.broadcast_to(adv[:, 0:1], adv.shape)
    k = 1
    while k < n_rows:
        head = head + DECAY ** (LANES * k) * up_rows(head, k)
        k *= 2
    adv = adv + jnp.exp((LANES - lanes).astype(jnp.float32) * LOG_DECAY) * up_rows(head, 1)
    reach = jnp.exp((seq - 1 - pos).astype(jnp.float32) * LOG_DECAY)

    m_adv = mask * adv
    m_reach = mask * reach
    at_zero = lanes[0:1] == 0
    parts = [mask, m_adv, m_reach, m_adv * adv, m_adv * reach, m_reach * reach]
    parts = [jnp.sum(a, axis=0, keepdims=True) for a in parts]
    parts += [jnp.where(at_zero, val[0:1], 0.0), jnp.where(at_zero, adv[0:1], 0.0)]
    note = jnp.sum(jnp.concatenate(parts, axis=0), axis=1, keepdims=True)
    note = jnp.broadcast_to(note, (8, LANES))
    send[...] = note
    recv[me] = note

    pl.semaphore_wait(barrier, n_dev - 1)
    copies = []
    for k in range(1, n_dev):
        copies.append(pltpu.make_async_remote_copy(
            src_ref=send, dst_ref=recv.at[me], send_sem=send_sem.at[k], recv_sem=recv_sem.at[k],
            device_id=peer(k), device_id_type=pl.DeviceIdType.MESH))
    for copy in copies:
        copy.start()
    for copy in copies:
        copy.wait()

    zero = jnp.zeros((1, LANES), jnp.float32)
    count, total, square, mine = zero, zero, zero, zero
    for dp in range(dp_size):
        carry = zero
        for cp in reversed(range(cp_size)):
            q = recv[dp * cp_size + cp]
            count = count + q[0:1]
            total = total + q[1:2] + carry * q[2:3]
            square = square + q[3:4] + carry * (2.0 * q[4:5] + carry * q[5:6])
            mine = jnp.where(me == dp * cp_size + cp, carry, mine)
            carry = DISCOUNT * q[6:7] + DECAY * (q[7:8] + DECAY ** (seq - 1) * carry)
    mean = total / count
    inv = lax.rsqrt(square / count - mean * mean + WHITEN_EPS)
    adv = adv + reach * mine
    ret_ref[...] = mask * (adv + val)
    white_ref[...] = mask * (adv - mean) * inv


def tail(dp_size, cp_size, val, rew, mask):
    vmem = pl.BlockSpec(memory_space=pltpu.VMEM)
    shape = jax.ShapeDtypeStruct(val.shape, jnp.float32)
    n_dev = dp_size * cp_size
    return pl.pallas_call(
        functools.partial(tail_kernel, dp_size, cp_size),
        out_shape=(shape, shape),
        in_specs=[vmem] * 3,
        out_specs=(vmem, vmem),
        scratch_shapes=[
            pltpu.VMEM((8, LANES), jnp.float32),
            pltpu.VMEM((n_dev, 8, LANES), jnp.float32),
            pltpu.SemaphoreType.DMA((n_dev,)),
            pltpu.SemaphoreType.DMA((n_dev,)),
        ],
        compiler_params=pltpu.CompilerParams(collective_id=0, has_side_effects=True),
        name="gae_tail",
    )(val, rew, mask)


def solution(mesh):
    dp_size, cp_size = mesh.shape['dp'], mesh.shape['cp']

    def local_step(x_blk, norm_gain, w_gate, w_up, w_down, final_gain, w_value, b_value, rew_blk, mask_blk):
        shape = rew_blk.shape
        fold = (shape[1] // LANES, LANES)
        mask2 = mask_blk.reshape(fold)
        val = mlp_values(mask2, norm_gain, final_gain, w_value, b_value, x_blk[0], w_gate, w_up, w_down)
        ret, white = tail(dp_size, cp_size, val, rew_blk.reshape(fold), mask2)
        return val.reshape(shape), ret.reshape(shape), white.reshape(shape)

    tok_spec = P('dp', 'cp')
    in_specs = (P('dp', 'cp', None), P(None), P(None, None), P(None, None), P(None, None), P(None), P(None), P(), tok_spec, tok_spec)
    return jax.shard_map(local_step, mesh=mesh, in_specs=in_specs, out_specs=(tok_spec, tok_spec, tok_spec), check_vma=False)
```

```python
import math
import functools
import jax
import jax.numpy as jnp
from jax import lax
from jax.sharding import PartitionSpec as P
from jax.experimental import pallas as pl
from jax.experimental.pallas import tpu as pltpu

NORM_EPS = 1e-6
WHITEN_EPS = 1e-8
DISCOUNT = 1.0
GAE_LAMBDA = 0.995
LOG_DECAY = math.log(DISCOUNT * GAE_LAMBDA)
DECAY = DISCOUNT * GAE_LAMBDA
LANES = 128
COLS = 512
LOAD_COLS = 1024
GROUP = 16
BIG = 256
SMALL = 128


def chunks(total, step):
    head = total % step
    starts = ([0] if head else []) + list(range(head, total, step))
    return [(start, end - start) for start, end in zip(starts, starts[1:] + [total])]


def in_hbm(x):
    return pltpu.with_memory_space_constraint(x, pltpu.HBM)


def hull(mask, parity):
    rows = lax.broadcasted_iota(jnp.int32, mask.shape, 0)
    lanes = lax.broadcasted_iota(jnp.int32, mask.shape, 1)
    group = rows * (LANES // GROUP) + lanes // GROUP
    live = (mask > 0) & (lax.rem(group, 2) == parity)
    pair = group // 2
    first = jnp.min(jnp.where(live, pair, mask.size))
    last = jnp.max(jnp.where(live, pair, -1))
    return first, jnp.maximum(last - first + 1, 0)


def prep_kernel(mask_hbm, x_hbm, out_hbm, mask_v, x_v, out_v, note_v, in_sem, out_sem, mask_sem):
    pairs, _, group, dim = x_hbm.shape
    steps = x_v.shape[0]
    span = pairs // steps

    def load(i):
        body = span - 1 if i == steps - 1 else span
        return pltpu.make_async_copy(x_hbm.at[pl.ds(i * span, body), 1], x_v.at[i, pl.ds(0, body)], in_sem.at[i])

    last_load = pltpu.make_async_copy(x_hbm.at[pairs - 1, 1], x_v.at[steps - 1, span - 1], in_sem.at[steps])

    def store(i):
        return pltpu.make_async_copy(out_v.at[i], out_hbm.at[pl.ds(i * span, span)], out_sem.at[i])

    mask_copy = pltpu.make_async_copy(mask_hbm, mask_v, mask_sem)
    mask_copy.start()
    for i in range(steps):
        load(i).start()
    last_load.start()
    mask_copy.wait()
    first, count = hull(mask_v[...], 1)
    row = lax.broadcasted_iota(jnp.int32, (group, dim), 0)
    note_v[...] = jnp.where(row < group // 2, first, count).astype(jnp.float32)
    note = pltpu.make_async_copy(note_v, out_hbm.at[pairs], out_sem.at[steps])
    note.start()
    for i in range(steps):
        load(i).wait()
        if i == steps - 1:
            last_load.wait()
        out_v[i] = x_v[i].astype(jnp.float32)
        store(i).start()
    for i in range(steps):
        store(i).wait()
    note.wait()


def prep(mask2, x4):
    pairs, _, group, dim = x4.shape
    steps = 8
    return pl.pallas_call(
        prep_kernel,
        out_shape=jax.ShapeDtypeStruct((pairs + 1, group, dim), jnp.float32),
        in_specs=[pl.BlockSpec(memory_space=pl.ANY), pl.BlockSpec(memory_space=pl.ANY)],
        out_specs=pl.BlockSpec(memory_space=pl.ANY),
        scratch_shapes=[
            pltpu.VMEM(mask2.shape, jnp.int32),
            pltpu.VMEM((steps, pairs // steps, group, dim), jnp.bfloat16),
            pltpu.VMEM((steps, pairs // steps, group, dim), jnp.float32),
            pltpu.VMEM((group, dim), jnp.float32),
            pltpu.SemaphoreType.DMA((steps + 1,)),
            pltpu.SemaphoreType.DMA((steps + 1,)),
            pltpu.SemaphoreType.DMA,
        ],
        name="widen_half",
    )(in_hbm(mask2), in_hbm(x4))


def mlp_block(rows, offset, x_f32, vecs, n_v, u_v, wg_v, wu_v):
    gain_ref = vecs[0]
    dim = x_f32.shape[-1]
    scale = lax.rsqrt(jnp.mean(x_f32 * x_f32, axis=-1, keepdims=True) + NORM_EPS)
    n_v[pl.ds(offset, rows), :] = (x_f32 * scale * gain_ref[...].reshape(1, dim)).astype(jnp.bfloat16)


def up_chunk(rows, offset, c, w, n_v, u_v, wg_v, wu_v):
    n = n_v[pl.ds(offset, rows), :]
    gate = jnp.dot(n, wg_v[:, c:c + w], preferred_element_type=jnp.float32)
    up = jnp.dot(n, wu_v[:, c:c + w], preferred_element_type=jnp.float32)
    u_v[pl.ds(offset, rows), c:c + w] = (jax.nn.silu(gate) * up).astype(jnp.bfloat16)


def head_value(rows, offset, x_f32, vecs, u_v, wd_v):
    _, final_ref, wval_ref, bias_ref = vecs
    dim = x_f32.shape[-1]
    h = x_f32 + jnp.dot(u_v[pl.ds(offset, rows), :], wd_v[...], preferred_element_type=jnp.float32)
    square = jnp.mean(h * h, axis=-1, keepdims=True)
    proj = jnp.sum(h * (final_ref[...] * wval_ref[...]).reshape(1, dim), axis=-1, keepdims=True)
    val = proj * lax.rsqrt(square + NORM_EPS) + bias_ref[...]
    return jnp.broadcast_to(val, (rows, LANES))


def mlp_kernel(load_weights, *refs):
    vecs_hbm, x_hbm, refs = refs[:4], refs[4], refs[5:]
    if load_weights:
        mask_hbm, wg_hbm, wu_hbm, wd_hbm, out_ref, wg_v, wu_v, wd_v, *refs = refs
        *vecs, x_v, n_v, u_v, val_v, vec_sem, x_sem, mask_v, mask_sem, w_sem, d_sem = refs
        parity, pairs, dim = 0, x_hbm.shape[0], x_hbm.shape[-1]
    else:
        wg_v, wu_v, wd_v, out_ref, *refs = refs
        *vecs, x_v, n_v, u_v, val_v, vec_sem, x_sem, note_v, note_sem = refs
        parity, pairs, dim = 1, x_hbm.shape[0] - 1, x_hbm.shape[-1]
    ffn = wg_v.shape[1]
    cols = chunks(ffn, COLS)
    loads = chunks(ffn, LOAD_COLS)
    big, small = BIG // GROUP, SMALL // GROUP

    vec_copies = []
    vecs = vecs_hbm

    if load_weights:
        mask_copy = pltpu.make_async_copy(mask_hbm, mask_v, mask_sem)
        mask_copy.start()

        def up_copies(i):
            c, w = loads[i]
            return (pltpu.make_async_copy(wg_hbm.at[:, pl.ds(c, w)], wg_v.at[:, pl.ds(c, w)], w_sem.at[0, i]),
                    pltpu.make_async_copy(wu_hbm.at[:, pl.ds(c, w)], wu_v.at[:, pl.ds(c, w)], w_sem.at[1, i]))

        down_copy = pltpu.make_async_copy(wd_hbm, wd_v, d_sem)
        for copy in up_copies(0):
            copy.start()
        for copy in vec_copies:
            copy.start()
        mask_copy.wait()
        first, count = hull(mask_v[...], parity)
    else:
        note = pltpu.make_async_copy(x_hbm.at[pairs], note_v, note_sem)
        note.start()
        for copy in vec_copies:
            copy.start()
        note.wait()
        first = jnp.max(note_v[0:GROUP // 2, 0:LANES]).astype(jnp.int32)
        count = jnp.max(note_v[GROUP // 2:GROUP, 0:LANES]).astype(jnp.int32)

    n_big = (count + small - 1) // big
    has_small = count > n_big * big

    def start_of(b, size):
        return jnp.minimum(first + b * big, pairs - size)

    def x_copy(b, size):
        where = pl.ds(start_of(b, size), size)
        src = x_hbm.at[where, 0] if load_weights else x_hbm.at[where]
        return pltpu.make_async_copy(src, x_v.at[b, pl.ds(0, size)], x_sem.at[b])

    def x_rows(b, size):
        return x_v[b, pl.ds(0, size)].reshape(size * GROUP, dim).astype(jnp.float32)

    def blocks(items, waits):
        offset = 0
        places = []
        for b, size in items:
            x_copy(b, size).wait()
            mlp_block(size * GROUP, offset, x_rows(b, size), vecs, n_v, u_v, wg_v, wu_v)
            places.append((b, size, offset))
            offset += size * GROUP
        for c, w in cols:
            for i, (first_col, _) in enumerate(loads):
                if waits and first_col == c:
                    for copy in up_copies(i):
                        copy.wait()
            for b, size, offset in places:
                up_chunk(size * GROUP, offset, c, w, n_v, u_v, wg_v, wu_v)
        if waits:
            down_copy.wait()
        for b, size, offset in places:
            val = head_value(size * GROUP, offset, x_rows(b, size), vecs, u_v, wd_v)
            base = start_of(b, size)
            for j in range(size):
                at = pl.multiple_of((base + j) * (2 * GROUP) + parity * GROUP, GROUP)
                val_v[pl.ds(at, GROUP), :] = val[j * GROUP:(j + 1) * GROUP]

    for b in range(pairs // big):
        @pl.when(b < n_big)
        def _():
            x_copy(b, big).start()

    @pl.when(has_small)
    def _():
        x_copy(n_big, small).start()

    for copy in vec_copies:
        copy.wait()

    if load_weights:
        for i in range(1, len(loads)):
            for copy in up_copies(i):
                copy.start()
        down_copy.start()

        @pl.when(n_big >= 2)
        def _():
            blocks([(0, big), (1, big)], True)

        @pl.when(n_big < 2)
        def _():
            for i in range(len(loads)):
                for copy in up_copies(i):
                    copy.wait()
            down_copy.wait()

    @pl.loop(jnp.where(n_big >= 2, 2, 0) if load_weights else 0, n_big)
    def _(b):
        blocks([(b, big)], False)

    @pl.when(has_small)
    def _():
        blocks([(n_big, small)], False)

    eye = lax.broadcasted_iota(jnp.int32, (LANES, LANES), 0) == lax.broadcasted_iota(jnp.int32, (LANES, LANES), 1)
    for r in range(out_ref.shape[0]):
        out_ref[r:r + 1, :] = jnp.sum(jnp.where(eye, val_v[r * LANES:(r + 1) * LANES, :], 0.0), axis=0, keepdims=True)


def mlp_call(load_weights, mask2, vecs, x, weights):
    vmem = pl.BlockSpec(memory_space=pltpu.VMEM)
    hbm = pl.BlockSpec(memory_space=pl.ANY)
    dim, ffn = weights[0].shape
    pairs = mask2.size // (2 * GROUP)
    out_shape = [jax.ShapeDtypeStruct(mask2.shape, jnp.float32)]
    if load_weights:
        out_shape += [pltpu.VMEM(w.shape, w.dtype) for w in weights]
    max_rows = 2 * BIG if load_weights else BIG
    scratch = [pltpu.VMEM((dim,), jnp.float32)] * 3 + [
        pltpu.VMEM((1, 1), jnp.float32),
        pltpu.VMEM((pairs * GROUP // BIG + 1, BIG // GROUP, GROUP, dim), x.dtype),
        pltpu.VMEM((max_rows, dim), jnp.bfloat16),
        pltpu.VMEM((max_rows, ffn), jnp.bfloat16),
        pltpu.VMEM((mask2.size, LANES), jnp.float32),
        pltpu.SemaphoreType.DMA((4,)),
        pltpu.SemaphoreType.DMA((pairs * GROUP // BIG + 1,)),
    ]
    if load_weights:
        n_loads = len(chunks(ffn, LOAD_COLS))
        scratch += [pltpu.VMEM(mask2.shape, jnp.int32), pltpu.SemaphoreType.DMA, pltpu.SemaphoreType.DMA((2, n_loads)), pltpu.SemaphoreType.DMA]
    else:
        scratch += [pltpu.VMEM((GROUP, dim), jnp.float32), pltpu.SemaphoreType.DMA]
    tokens = mask2.size // 2
    return pl.pallas_call(
        functools.partial(mlp_kernel, load_weights),
        out_shape=out_shape,
        in_specs=[vmem] * 4 + ([hbm] * 5 if load_weights else [hbm] + [vmem] * 3),
        out_specs=[vmem] * len(out_shape),
        scratch_shapes=scratch,
        compiler_params=pltpu.CompilerParams(vmem_limit_bytes=20 * 1024 * 1024),
        cost_estimate=pl.CostEstimate(flops=6 * tokens * dim * ffn, bytes_accessed=6 * dim * ffn, transcendentals=tokens * ffn),
        name="mlp_own" if load_weights else "mlp_sent",
    )(*[in_hbm(v) for v in vecs[:3]], vecs[3], in_hbm(x), *([in_hbm(v) for v in (mask2, *weights)] if load_weights else weights))


def tail_kernel(dp_size, cp_size, own_ref, sent_ref, rew_ref, mask_ref, val_ref, ret_ref, white_ref, send, recv, back, send_sem, recv_sem, back_sem):
    n_dev = dp_size * cp_size
    n_rows = own_ref.shape[0]
    seq = n_rows * LANES
    me = lax.axis_index('dp') * cp_size + lax.axis_index('cp')
    barrier = pltpu.get_barrier_semaphore()

    def peer(k):
        other = lax.rem(me + k, n_dev)
        return {'dp': other // cp_size, 'cp': lax.rem(other, cp_size)}

    for k in range(1, n_dev):
        pl.semaphore_signal(barrier, inc=1, device_id=peer(k), device_id_type=pl.DeviceIdType.MESH)

    cp = lax.axis_index('cp')
    partner = {'dp': lax.axis_index('dp'), 'cp': cp + 1 - 2 * lax.rem(cp, 2)}
    mask = mask_ref[...].astype(jnp.float32)
    rows = lax.broadcasted_iota(jnp.int32, mask.shape, 0)
    lanes = lax.broadcasted_iota(jnp.int32, mask.shape, 1)
    pl.semaphore_wait(barrier, n_dev - 1)
    give = pltpu.make_async_remote_copy(
        src_ref=sent_ref, dst_ref=back, send_sem=back_sem.at[0], recv_sem=back_sem.at[1],
        device_id=partner, device_id_type=pl.DeviceIdType.MESH)
    give.start()
    give.wait()
    is_own = lax.rem(lanes // GROUP, 2) == 0
    val = jnp.where(mask > 0, jnp.where(is_own, own_ref[...], back[...]), 0.0)
    val_ref[...] = val
    pos = rows * LANES + lanes

    def up_rows(a, k):
        return jnp.where(rows < n_rows - k, pltpu.roll(a, n_rows - k, 0), 0.0)

    shifted = pltpu.roll(val, LANES - 1, 1)
    next_val = jnp.where(lanes < LANES - 1, shifted, up_rows(shifted, 1))
    adv = mask * rew_ref[...] + DISCOUNT * next_val - val
    k = 1
    while k < LANES:
        adv = adv + DECAY ** k * jnp.where(lanes < LANES - k, pltpu.roll(adv, LANES - k, 1), 0.0)
        k *= 2
    head = jnp.broadcast_to(adv[:, 0:1], adv.shape)
    k = 1
    while k < n_rows:
        head = head + DECAY ** (LANES * k) * up_rows(head, k)
        k *= 2
    adv = adv + jnp.exp((LANES - lanes).astype(jnp.float32) * LOG_DECAY) * up_rows(head, 1)
    reach = jnp.exp((seq - 1 - pos).astype(jnp.float32) * LOG_DECAY)

    m_adv = mask * adv
    m_reach = mask * reach
    at_zero = lanes[0:1] == 0
    parts = [mask, m_adv, m_reach, m_adv * adv, m_adv * reach, m_reach * reach]
    parts = [jnp.sum(a, axis=0, keepdims=True) for a in parts]
    parts += [jnp.where(at_zero, val[0:1], 0.0), jnp.where(at_zero, adv[0:1], 0.0)]
    note = jnp.sum(jnp.concatenate(parts, axis=0), axis=1, keepdims=True)
    note = jnp.broadcast_to(note, (8, LANES))
    send[...] = note
    recv[me] = note

    copies = []
    for k in range(1, n_dev):
        copies.append(pltpu.make_async_remote_copy(
            src_ref=send, dst_ref=recv.at[me], send_sem=send_sem.at[k], recv_sem=recv_sem.at[k],
            device_id=peer(k), device_id_type=pl.DeviceIdType.MESH))
    for copy in copies:
        copy.start()
    for copy in copies:
        copy.wait()

    zero = jnp.zeros((1, LANES), jnp.float32)
    count, total, square, mine = zero, zero, zero, zero
    for dp in range(dp_size):
        carry = zero
        for cp in reversed(range(cp_size)):
            q = recv[dp * cp_size + cp]
            count = count + q[0:1]
            total = total + q[1:2] + carry * q[2:3]
            square = square + q[3:4] + carry * (2.0 * q[4:5] + carry * q[5:6])
            mine = jnp.where(me == dp * cp_size + cp, carry, mine)
            carry = DISCOUNT * q[6:7] + DECAY * (q[7:8] + DECAY ** (seq - 1) * carry)
    mean = total / count
    inv = lax.rsqrt(square / count - mean * mean + WHITEN_EPS)
    adv = adv + reach * mine
    ret_ref[...] = adv + val
    white_ref[...] = (adv - mean) * inv


def tail(dp_size, cp_size, own, sent, rew, mask):
    vmem = pl.BlockSpec(memory_space=pltpu.VMEM)
    shape = jax.ShapeDtypeStruct(own.shape, jnp.float32)
    n_dev = dp_size * cp_size
    return pl.pallas_call(
        functools.partial(tail_kernel, dp_size, cp_size),
        out_shape=(shape, shape, shape),
        in_specs=[vmem] * 4,
        out_specs=(vmem, vmem, vmem),
        scratch_shapes=[
            pltpu.VMEM((8, LANES), jnp.float32),
            pltpu.VMEM((n_dev, 8, LANES), jnp.float32),
            pltpu.VMEM(own.shape, jnp.float32),
            pltpu.SemaphoreType.DMA((n_dev,)),
            pltpu.SemaphoreType.DMA((n_dev,)),
            pltpu.SemaphoreType.DMA((2,)),
        ],
        compiler_params=pltpu.CompilerParams(collective_id=0, has_side_effects=True, vmem_limit_bytes=4 * 1024 * 1024),
        name="gae_tail",
    )(own, sent, rew, mask)


def solution(mesh):
    dp_size, cp_size = mesh.shape['dp'], mesh.shape['cp']

    swap = [(i, i ^ 1) for i in range(cp_size)]

    def local_step(x_blk, norm_gain, w_gate, w_up, w_down, final_gain, w_value, b_value, rew_blk, mask_blk):
        shape = rew_blk.shape
        fold = (shape[1] // LANES, LANES)
        mask2 = mask_blk.reshape(fold)
        x4 = x_blk.reshape(shape[1] // (2 * GROUP), 2, GROUP, x_blk.shape[-1])
        vecs = (norm_gain, final_gain, w_value, b_value.reshape(1, 1))
        recv = lax.ppermute(prep(mask2, x4), 'cp', swap)
        own, *weights = mlp_call(True, mask2, vecs, x4, (w_gate, w_up, w_down))
        sent, = mlp_call(False, mask2, vecs, recv, weights)
        val, ret, white = tail(dp_size, cp_size, own, sent, rew_blk.reshape(fold), mask2)
        mask_f = mask_blk.astype(jnp.float32)
        return mask_f * val.reshape(shape), mask_f * ret.reshape(shape), mask_f * white.reshape(shape)

    tok_spec = P('dp', 'cp')
    in_specs = (P('dp', 'cp', None), P(None), P(None, None), P(None, None), P(None, None), P(None), P(None), P(), tok_spec, tok_spec)
    return jax.shard_map(local_step, mesh=mesh, in_specs=in_specs, out_specs=(tok_spec, tok_spec, tok_spec), check_vma=False)
```

```python
import math
import functools
import jax
import jax.numpy as jnp
from jax import lax
from jax.sharding import PartitionSpec as P
from jax.experimental import pallas as pl
from jax.experimental.pallas import tpu as pltpu

NORM_EPS = 1e-6
WHITEN_EPS = 1e-8
DISCOUNT = 1.0
GAE_LAMBDA = 0.995
LOG_DECAY = math.log(DISCOUNT * GAE_LAMBDA)
DECAY = DISCOUNT * GAE_LAMBDA
LANES = 128
COLS = 512
LOAD_COLS = 1024
GROUP = 16
BIG = 256
SMALL = 128


def chunks(total, step):
    head = total % step
    starts = ([0] if head else []) + list(range(head, total, step))
    return [(start, end - start) for start, end in zip(starts, starts[1:] + [total])]


def in_hbm(x):
    return pltpu.with_memory_space_constraint(x, pltpu.HBM)


def hull(mask, parity):
    rows = lax.broadcasted_iota(jnp.int32, mask.shape, 0)
    lanes = lax.broadcasted_iota(jnp.int32, mask.shape, 1)
    group = rows * (LANES // GROUP) + lanes // GROUP
    live = (mask > 0) & (lax.rem(group, 2) == parity)
    pair = group // 2
    first = jnp.min(jnp.where(live, pair, mask.size))
    last = jnp.max(jnp.where(live, pair, -1))
    return first, jnp.maximum(last - first + 1, 0)


def prep_kernel(mask_hbm, x_hbm, out_hbm, mask_v, x_v, out_v, note_v, in_sem, out_sem, mask_sem):
    pairs, _, group, dim = x_hbm.shape
    steps = x_v.shape[0]
    span = pairs // steps

    def load(i):
        body = span - 1 if i == steps - 1 else span
        return pltpu.make_async_copy(x_hbm.at[pl.ds(i * span, body), 1], x_v.at[i, pl.ds(0, body)], in_sem.at[i])

    last_load = pltpu.make_async_copy(x_hbm.at[pairs - 1, 1], x_v.at[steps - 1, span - 1], in_sem.at[steps])

    def store(i):
        return pltpu.make_async_copy(out_v.at[i], out_hbm.at[pl.ds(i * span, span)], out_sem.at[i])

    mask_copy = pltpu.make_async_copy(mask_hbm, mask_v, mask_sem)
    mask_copy.start()
    for i in range(steps):
        load(i).start()
    last_load.start()
    for i in range(steps):
        load(i).wait()
        if i == steps - 1:
            last_load.wait()
        out_v[i] = x_v[i].astype(jnp.float32)
        store(i).start()
    mask_copy.wait()
    first, count = hull(mask_v[...], 1)
    row = lax.broadcasted_iota(jnp.int32, (group, dim), 0)
    note_v[...] = jnp.where(row < group // 2, first, count).astype(jnp.float32)
    note = pltpu.make_async_copy(note_v, out_hbm.at[pairs], out_sem.at[steps])
    note.start()
    for i in range(steps):
        store(i).wait()
    note.wait()


def prep(mask2, x4):
    pairs, _, group, dim = x4.shape
    steps = 8
    return pl.pallas_call(
        prep_kernel,
        out_shape=jax.ShapeDtypeStruct((pairs + 1, group, dim), jnp.float32),
        in_specs=[pl.BlockSpec(memory_space=pl.ANY), pl.BlockSpec(memory_space=pl.ANY)],
        out_specs=pl.BlockSpec(memory_space=pl.ANY),
        scratch_shapes=[
            pltpu.VMEM(mask2.shape, jnp.int32),
            pltpu.VMEM((steps, pairs // steps, group, dim), jnp.bfloat16),
            pltpu.VMEM((steps, pairs // steps, group, dim), jnp.float32),
            pltpu.VMEM((group, dim), jnp.float32),
            pltpu.SemaphoreType.DMA((steps + 1,)),
            pltpu.SemaphoreType.DMA((steps + 1,)),
            pltpu.SemaphoreType.DMA,
        ],
        name="widen_half",
    )(in_hbm(mask2), in_hbm(x4))


def mlp_block(rows, offset, x_f32, vecs, n_v, u_v, wg_v, wu_v):
    gain_ref = vecs[0]
    dim = x_f32.shape[-1]
    scale = lax.rsqrt(jnp.mean(x_f32 * x_f32, axis=-1, keepdims=True) + NORM_EPS)
    n_v[pl.ds(offset, rows), :] = (x_f32 * scale * gain_ref[...].reshape(1, dim)).astype(jnp.bfloat16)


def up_chunk(rows, offset, c, w, n_v, u_v, wg_v, wu_v):
    n = n_v[pl.ds(offset, rows), :]
    gate = jnp.dot(n, wg_v[:, c:c + w], preferred_element_type=jnp.float32)
    up = jnp.dot(n, wu_v[:, c:c + w], preferred_element_type=jnp.float32)
    u_v[pl.ds(offset, rows), c:c + w] = (jax.nn.silu(gate) * up).astype(jnp.bfloat16)


def head_value(rows, offset, x_f32, vecs, u_v, wd_v):
    _, final_ref, wval_ref, bias_ref = vecs
    dim = x_f32.shape[-1]
    h = x_f32 + jnp.dot(u_v[pl.ds(offset, rows), :], wd_v[...], preferred_element_type=jnp.float32)
    square = jnp.mean(h * h, axis=-1, keepdims=True)
    proj = jnp.sum(h * (final_ref[...] * wval_ref[...]).reshape(1, dim), axis=-1, keepdims=True)
    val = proj * lax.rsqrt(square + NORM_EPS) + bias_ref[...]
    return jnp.broadcast_to(val, (rows, LANES))


def mlp_kernel(load_weights, *refs):
    vecs_hbm, x_hbm, refs = refs[:4], refs[4], refs[5:]
    if load_weights:
        mask_hbm, wg_hbm, wu_hbm, wd_hbm, out_ref, wg_v, wu_v, wd_v, *refs = refs
        *vecs, x_v, n_v, u_v, val_v, vec_sem, x_sem, mask_v, mask_sem, w_sem, d_sem = refs
        parity, pairs, dim = 0, x_hbm.shape[0], x_hbm.shape[-1]
    else:
        wg_v, wu_v, wd_v, out_ref, *refs = refs
        *vecs, x_v, n_v, u_v, val_v, vec_sem, x_sem, note_v, note_sem = refs
        parity, pairs, dim = 1, x_hbm.shape[0] - 1, x_hbm.shape[-1]
    ffn = wg_v.shape[1]
    cols = chunks(ffn, COLS)
    loads = chunks(ffn, LOAD_COLS)
    big, small = BIG // GROUP, SMALL // GROUP

    vec_copies = [pltpu.make_async_copy(src, dst.at[pl.ds(0, dim)], vec_sem.at[i]) for i, (src, dst) in enumerate(zip(vecs_hbm[:3], vecs[:3]))]
    vecs = [*[v.at[pl.ds(0, dim)] for v in vecs[:3]], vecs_hbm[3]]

    if load_weights:
        mask_copy = pltpu.make_async_copy(mask_hbm, mask_v, mask_sem)
        mask_copy.start()

        def up_copies(i):
            c, w = loads[i]
            return (pltpu.make_async_copy(wg_hbm.at[:, pl.ds(c, w)], wg_v.at[:, pl.ds(c, w)], w_sem.at[0, i]),
                    pltpu.make_async_copy(wu_hbm.at[:, pl.ds(c, w)], wu_v.at[:, pl.ds(c, w)], w_sem.at[1, i]))

        down_copy = pltpu.make_async_copy(wd_hbm, wd_v, d_sem)
        for copy in up_copies(0):
            copy.start()
        for copy in vec_copies:
            copy.start()
        mask_copy.wait()
        first, count = hull(mask_v[...], parity)
    else:
        note = pltpu.make_async_copy(x_hbm.at[pairs], note_v, note_sem)
        note.start()
        for copy in vec_copies:
            copy.start()
        note.wait()
        first = jnp.max(note_v[0:GROUP // 2, 0:LANES]).astype(jnp.int32)
        count = jnp.max(note_v[GROUP // 2:GROUP, 0:LANES]).astype(jnp.int32)

    n_big = (count + small - 1) // big
    has_small = count > n_big * big

    def start_of(b, size):
        return jnp.minimum(first + b * big, pairs - size)

    def x_copy(b, size):
        where = pl.ds(start_of(b, size), size)
        src = x_hbm.at[where, 0] if load_weights else x_hbm.at[where]
        return pltpu.make_async_copy(src, x_v.at[b, pl.ds(0, size)], x_sem.at[b])

    def x_rows(b, size):
        return x_v[b, pl.ds(0, size)].reshape(size * GROUP, dim).astype(jnp.float32)

    def blocks(items, waits):
        offset = 0
        places = []
        for b, size in items:
            x_copy(b, size).wait()
            mlp_block(size * GROUP, offset, x_rows(b, size), vecs, n_v, u_v, wg_v, wu_v)
            places.append((b, size, offset))
            offset += size * GROUP
        for c, w in cols:
            for i, (first_col, _) in enumerate(loads):
                if waits and first_col == c:
                    for copy in up_copies(i):
                        copy.wait()
            for b, size, offset in places:
                up_chunk(size * GROUP, offset, c, w, n_v, u_v, wg_v, wu_v)
        if waits:
            down_copy.wait()
        for b, size, offset in places:
            val = head_value(size * GROUP, offset, x_rows(b, size), vecs, u_v, wd_v)
            base = start_of(b, size)
            for j in range(size):
                at = pl.multiple_of((base + j) * (2 * GROUP) + parity * GROUP, GROUP)
                val_v[pl.ds(at, GROUP), :] = val[j * GROUP:(j + 1) * GROUP]

    for b in range(pairs // big):
        @pl.when(b < n_big)
        def _():
            x_copy(b, big).start()

    @pl.when(has_small)
    def _():
        x_copy(n_big, small).start()

    for copy in vec_copies:
        copy.wait()

    if load_weights:
        for i in range(1, len(loads)):
            for copy in up_copies(i):
                copy.start()
        down_copy.start()

        @pl.when(n_big >= 2)
        def _():
            blocks([(0, big), (1, big)], True)

        @pl.when(n_big < 2)
        def _():
            for i in range(len(loads)):
                for copy in up_copies(i):
                    copy.wait()
            down_copy.wait()

    @pl.loop(jnp.where(n_big >= 2, 2, 0) if load_weights else 0, n_big)
    def _(b):
        blocks([(b, big)], False)

    @pl.when(has_small)
    def _():
        blocks([(n_big, small)], False)

    eye = lax.broadcasted_iota(jnp.int32, (LANES, LANES), 0) == lax.broadcasted_iota(jnp.int32, (LANES, LANES), 1)
    for r in range(out_ref.shape[0]):
        out_ref[r:r + 1, :] = jnp.sum(jnp.where(eye, val_v[r * LANES:(r + 1) * LANES, :], 0.0), axis=0, keepdims=True)


def mlp_call(load_weights, mask2, vecs, x, weights):
    vmem = pl.BlockSpec(memory_space=pltpu.VMEM)
    hbm = pl.BlockSpec(memory_space=pl.ANY)
    dim, ffn = weights[0].shape
    pairs = mask2.size // (2 * GROUP)
    out_shape = [jax.ShapeDtypeStruct(mask2.shape, jnp.float32)]
    if load_weights:
        out_shape += [pltpu.VMEM(w.shape, w.dtype) for w in weights]
    max_rows = 2 * BIG if load_weights else BIG
    scratch = [pltpu.VMEM((-(-dim // 1024) * 1024,), jnp.float32)] * 3 + [
        pltpu.VMEM((1, 1), jnp.float32),
        pltpu.VMEM((pairs * GROUP // BIG + 1, BIG // GROUP, GROUP, dim), x.dtype),
        pltpu.VMEM((max_rows, dim), jnp.bfloat16),
        pltpu.VMEM((max_rows, ffn), jnp.bfloat16),
        pltpu.VMEM((mask2.size, LANES), jnp.float32),
        pltpu.SemaphoreType.DMA((4,)),
        pltpu.SemaphoreType.DMA((pairs * GROUP // BIG + 1,)),
    ]
    if load_weights:
        n_loads = len(chunks(ffn, LOAD_COLS))
        scratch += [pltpu.VMEM(mask2.shape, jnp.int32), pltpu.SemaphoreType.DMA, pltpu.SemaphoreType.DMA((2, n_loads)), pltpu.SemaphoreType.DMA]
    else:
        scratch += [pltpu.VMEM((GROUP, dim), jnp.float32), pltpu.SemaphoreType.DMA]
    tokens = mask2.size // 2
    return pl.pallas_call(
        functools.partial(mlp_kernel, load_weights),
        out_shape=out_shape,
        in_specs=[hbm] * 3 + [vmem] + ([hbm] * 5 if load_weights else [hbm] + [vmem] * 3),
        out_specs=[vmem] * len(out_shape),
        scratch_shapes=scratch,
        compiler_params=pltpu.CompilerParams(vmem_limit_bytes=20 * 1024 * 1024),
        cost_estimate=pl.CostEstimate(flops=6 * tokens * dim * ffn, bytes_accessed=6 * dim * ffn, transcendentals=tokens * ffn),
        name="mlp_own" if load_weights else "mlp_sent",
    )(*[in_hbm(v) for v in vecs[:3]], vecs[3], in_hbm(x), *([in_hbm(v) for v in (mask2, *weights)] if load_weights else weights))


def tail_kernel(dp_size, cp_size, own_ref, sent_ref, rew_ref, mask_ref, val_ref, ret_ref, white_ref, send, recv, back, send_sem, recv_sem, back_sem):
    n_dev = dp_size * cp_size
    n_rows = own_ref.shape[0]
    seq = n_rows * LANES
    me = lax.axis_index('dp') * cp_size + lax.axis_index('cp')
    barrier = pltpu.get_barrier_semaphore()

    def peer(k):
        other = lax.rem(me + k, n_dev)
        return {'dp': other // cp_size, 'cp': lax.rem(other, cp_size)}

    for k in range(1, n_dev):
        pl.semaphore_signal(barrier, inc=1, device_id=peer(k), device_id_type=pl.DeviceIdType.MESH)

    cp = lax.axis_index('cp')
    partner = {'dp': lax.axis_index('dp'), 'cp': cp + 1 - 2 * lax.rem(cp, 2)}
    mask = mask_ref[...].astype(jnp.float32)
    rows = lax.broadcasted_iota(jnp.int32, mask.shape, 0)
    lanes = lax.broadcasted_iota(jnp.int32, mask.shape, 1)
    pos = rows * LANES + lanes
    reward = mask * rew_ref[...]
    row_reach = jnp.exp((LANES - lanes).astype(jnp.float32) * LOG_DECAY)
    reach = jnp.exp((seq - 1 - pos).astype(jnp.float32) * LOG_DECAY)
    m_reach = mask * reach
    fixed = [jnp.sum(a, axis=0, keepdims=True) for a in (mask, m_reach, m_reach * reach)]
    is_own = lax.rem(lanes // GROUP, 2) == 0

    def up_rows(a, k):
        return jnp.where(rows < n_rows - k, pltpu.roll(a, n_rows - k, 0), 0.0)

    pl.semaphore_wait(barrier, n_dev - 1)
    give = pltpu.make_async_remote_copy(
        src_ref=sent_ref, dst_ref=back, send_sem=back_sem.at[0], recv_sem=back_sem.at[1],
        device_id=partner, device_id_type=pl.DeviceIdType.MESH)
    give.start()
    give.wait()
    val = jnp.where(mask > 0, jnp.where(is_own, own_ref[...], back[...]), 0.0)
    val_ref[...] = val

    shifted = pltpu.roll(val, LANES - 1, 1)
    next_val = jnp.where(lanes < LANES - 1, shifted, up_rows(shifted, 1))
    adv = reward + DISCOUNT * next_val - val
    k = 1
    while k < LANES:
        adv = adv + DECAY ** k * jnp.where(lanes < LANES - k, pltpu.roll(adv, LANES - k, 1), 0.0)
        k *= 2
    head = jnp.broadcast_to(adv[:, 0:1], adv.shape)
    k = 1
    while k < n_rows:
        head = head + DECAY ** (LANES * k) * up_rows(head, k)
        k *= 2
    adv = adv + row_reach * up_rows(head, 1)

    m_adv = mask * adv
    at_zero = lanes[0:1] == 0
    moving = [jnp.sum(a, axis=0, keepdims=True) for a in (m_adv, m_adv * adv, m_adv * reach)]
    parts = [fixed[0], moving[0], fixed[1], moving[1], moving[2], fixed[2]]
    parts += [jnp.where(at_zero, val[0:1], 0.0), jnp.where(at_zero, adv[0:1], 0.0)]
    note = jnp.sum(jnp.concatenate(parts, axis=0), axis=1, keepdims=True)
    note = jnp.broadcast_to(note, (8, LANES))
    send[...] = note
    recv[me] = note

    copies = []
    for k in range(1, n_dev):
        copies.append(pltpu.make_async_remote_copy(
            src_ref=send, dst_ref=recv.at[me], send_sem=send_sem.at[k], recv_sem=recv_sem.at[k],
            device_id=peer(k), device_id_type=pl.DeviceIdType.MESH))
    for copy in copies:
        copy.start()
    for copy in copies:
        copy.wait()

    zero = jnp.zeros((1, LANES), jnp.float32)
    count, total, square, mine = zero, zero, zero, zero
    for dp in range(dp_size):
        carry = zero
        for cp in reversed(range(cp_size)):
            q = recv[dp * cp_size + cp]
            count = count + q[0:1]
            total = total + q[1:2] + carry * q[2:3]
            square = square + q[3:4] + carry * (2.0 * q[4:5] + carry * q[5:6])
            mine = jnp.where(me == dp * cp_size + cp, carry, mine)
            carry = DISCOUNT * q[6:7] + DECAY * (q[7:8] + DECAY ** (seq - 1) * carry)
    mean = total / count
    inv = lax.rsqrt(square / count - mean * mean + WHITEN_EPS)
    adv = adv + reach * mine
    ret_ref[...] = adv + val
    white_ref[...] = (adv - mean) * inv


def tail(dp_size, cp_size, own, sent, rew, mask):
    vmem = pl.BlockSpec(memory_space=pltpu.VMEM)
    shape = jax.ShapeDtypeStruct(own.shape, jnp.float32)
    n_dev = dp_size * cp_size
    return pl.pallas_call(
        functools.partial(tail_kernel, dp_size, cp_size),
        out_shape=(shape, shape, shape),
        in_specs=[vmem] * 4,
        out_specs=(vmem, vmem, vmem),
        scratch_shapes=[
            pltpu.VMEM((8, LANES), jnp.float32),
            pltpu.VMEM((n_dev, 8, LANES), jnp.float32),
            pltpu.VMEM(own.shape, jnp.float32),
            pltpu.SemaphoreType.DMA((n_dev,)),
            pltpu.SemaphoreType.DMA((n_dev,)),
            pltpu.SemaphoreType.DMA((2,)),
        ],
        compiler_params=pltpu.CompilerParams(collective_id=0, has_side_effects=True, vmem_limit_bytes=4 * 1024 * 1024),
        name="gae_tail",
    )(own, sent, rew, mask)


def solution(mesh):
    dp_size, cp_size = mesh.shape['dp'], mesh.shape['cp']

    swap = [(i, i ^ 1) for i in range(cp_size)]

    def local_step(x_blk, norm_gain, w_gate, w_up, w_down, final_gain, w_value, b_value, rew_blk, mask_blk):
        shape = rew_blk.shape
        fold = (shape[1] // LANES, LANES)
        mask2 = mask_blk.reshape(fold)
        x4 = x_blk.reshape(shape[1] // (2 * GROUP), 2, GROUP, x_blk.shape[-1])
        vecs = (norm_gain, final_gain, w_value, b_value.reshape(1, 1))
        recv = lax.ppermute(prep(mask2, x4), 'cp', swap)
        own, *weights = mlp_call(True, mask2, vecs, x4, (w_gate, w_up, w_down))
        sent, = mlp_call(False, mask2, vecs, recv, weights)
        val, ret, white = tail(dp_size, cp_size, own, sent, rew_blk.reshape(fold), mask2)
        mask_f = mask_blk.astype(jnp.float32)
        return mask_f * val.reshape(shape), mask_f * ret.reshape(shape), mask_f * white.reshape(shape)

    tok_spec = P('dp', 'cp')
    in_specs = (P('dp', 'cp', None), P(None), P(None, None), P(None, None), P(None, None), P(None), P(None), P(), tok_spec, tok_spec)
    return jax.shard_map(local_step, mesh=mesh, in_specs=in_specs, out_specs=(tok_spec, tok_spec, tok_spec), check_vma=False)
```

```python
import math
import functools
import jax
import jax.numpy as jnp
from jax import lax
from jax.sharding import PartitionSpec as P
from jax.experimental import pallas as pl
from jax.experimental.pallas import tpu as pltpu

NORM_EPS = 1e-6
WHITEN_EPS = 1e-8
DISCOUNT = 1.0
GAE_LAMBDA = 0.995
LOG_DECAY = math.log(DISCOUNT * GAE_LAMBDA)
DECAY = DISCOUNT * GAE_LAMBDA
LANES = 128
COLS = 256
LOAD_COLS = 1024
GROUP = 16
BIG = 256
SMALL = 128


def chunks(total, step):
    head = total % step
    starts = ([0] if head else []) + list(range(head, total, step))
    return [(start, end - start) for start, end in zip(starts, starts[1:] + [total])]


def in_hbm(x):
    return pltpu.with_memory_space_constraint(x, pltpu.HBM)


def hull(mask, parity):
    rows = lax.broadcasted_iota(jnp.int32, mask.shape, 0)
    lanes = lax.broadcasted_iota(jnp.int32, mask.shape, 1)
    group = rows * (LANES // GROUP) + lanes // GROUP
    live = (mask > 0) & (lax.rem(group, 2) == parity)
    pair = group // 2
    first = jnp.min(jnp.where(live, pair, mask.size))
    last = jnp.max(jnp.where(live, pair, -1))
    return first, jnp.maximum(last - first + 1, 0)


def prep_kernel(mask_hbm, x_hbm, out_hbm, span_ref, mask_v, x_v, out_v, note_v, in_sem, out_sem, mask_sem):
    pairs, _, group, dim = x_hbm.shape
    steps = x_v.shape[0]
    span = pairs // steps

    def load(i):
        body = span - 1 if i == steps - 1 else span
        return pltpu.make_async_copy(x_hbm.at[pl.ds(i * span, body), 1], x_v.at[i, pl.ds(0, body)], in_sem.at[i])

    last_load = pltpu.make_async_copy(x_hbm.at[pairs - 1, 1], x_v.at[steps - 1, span - 1], in_sem.at[steps])

    def store(i):
        return pltpu.make_async_copy(out_v.at[i], out_hbm.at[pl.ds(i * span, span)], out_sem.at[i])

    mask_copy = pltpu.make_async_copy(mask_hbm, mask_v, mask_sem)
    mask_copy.start()
    for i in range(steps):
        load(i).start()
    last_load.start()
    for i in range(steps):
        load(i).wait()
        if i == steps - 1:
            last_load.wait()
        out_v[i] = x_v[i].astype(jnp.float32)
        store(i).start()
    mask_copy.wait()
    first, count = hull(mask_v[...], 1)
    row = lax.broadcasted_iota(jnp.int32, (group, dim), 0)
    note_v[...] = jnp.where(row < group // 2, first, count).astype(jnp.float32)
    note = pltpu.make_async_copy(note_v, out_hbm.at[pairs], out_sem.at[steps])
    note.start()
    first, count = hull(mask_v[...], 0)
    row = lax.broadcasted_iota(jnp.int32, span_ref.shape, 0)
    span_ref[...] = jnp.where(row < group // 2, first, count)
    for i in range(steps):
        store(i).wait()
    note.wait()


def prep(mask2, x4):
    pairs, _, group, dim = x4.shape
    steps = 8
    return pl.pallas_call(
        prep_kernel,
        out_shape=[jax.ShapeDtypeStruct((pairs + 1, group, dim), jnp.float32), pltpu.VMEM((group, LANES), jnp.int32)],
        in_specs=[pl.BlockSpec(memory_space=pl.ANY), pl.BlockSpec(memory_space=pl.ANY)],
        out_specs=[pl.BlockSpec(memory_space=pl.ANY), pl.BlockSpec(memory_space=pltpu.VMEM)],
        scratch_shapes=[
            pltpu.VMEM(mask2.shape, jnp.int32),
            pltpu.VMEM((steps, pairs // steps, group, dim), jnp.bfloat16),
            pltpu.VMEM((steps, pairs // steps, group, dim), jnp.float32),
            pltpu.VMEM((group, dim), jnp.float32),
            pltpu.SemaphoreType.DMA((steps + 1,)),
            pltpu.SemaphoreType.DMA((steps + 1,)),
            pltpu.SemaphoreType.DMA,
        ],
        compiler_params=pltpu.CompilerParams(vmem_limit_bytes=12 * 1024 * 1024),
        name="widen_half",
    )(in_hbm(mask2), in_hbm(x4))


def mlp_block(rows, offset, x_f32, vecs, n_v, u_v, wg_v, wu_v):
    gain_ref = vecs[0]
    dim = x_f32.shape[-1]
    scale = lax.rsqrt(jnp.mean(x_f32 * x_f32, axis=-1, keepdims=True) + NORM_EPS)
    n_v[pl.ds(offset, rows), :] = (x_f32 * scale * gain_ref[...].reshape(1, dim)).astype(jnp.bfloat16)


def up_chunk(rows, offset, c, w, n_v, u_v, wg_v, wu_v):
    n = n_v[pl.ds(offset, rows), :]
    gate = jnp.dot(n, wg_v[:, c:c + w], preferred_element_type=jnp.float32)
    up = jnp.dot(n, wu_v[:, c:c + w], preferred_element_type=jnp.float32)
    u_v[pl.ds(offset, rows), c:c + w] = (jax.nn.silu(gate) * up).astype(jnp.bfloat16)


def head_value(rows, offset, x_f32, vecs, u_v, wd_v):
    _, final_ref, wval_ref = vecs
    dim = x_f32.shape[-1]
    h = x_f32 + jnp.dot(u_v[pl.ds(offset, rows), :], wd_v[...], preferred_element_type=jnp.float32)
    square = jnp.mean(h * h, axis=-1, keepdims=True)
    proj = jnp.sum(h * (final_ref[...] * wval_ref[...]).reshape(1, dim), axis=-1, keepdims=True)
    val = proj * lax.rsqrt(square + NORM_EPS)
    return jnp.broadcast_to(val, (rows, LANES))


def mlp_kernel(load_weights, *refs):
    vecs_hbm, x_hbm, refs = refs[:3], refs[3], refs[4:]
    if load_weights:
        span_ref, wg_hbm, wu_hbm, wd_hbm, out_ref, wg_v, wu_v, wd_v, *refs = refs
        *vecs, x_v, n_v, u_v, val_v, vec_sem, x_sem, w_sem, d_sem = refs
        parity, pairs, dim = 0, x_hbm.shape[0], x_hbm.shape[-1]
    else:
        wg_v, wu_v, wd_v, out_ref, *refs = refs
        *vecs, x_v, n_v, u_v, val_v, vec_sem, x_sem, note_v, note_sem = refs
        parity, pairs, dim = 1, x_hbm.shape[0] - 1, x_hbm.shape[-1]
    ffn = wg_v.shape[1]
    cols = chunks(ffn, COLS)
    loads = chunks(ffn, LOAD_COLS)
    big, small = BIG // GROUP, SMALL // GROUP

    vec_copies = [pltpu.make_async_copy(src, dst.at[pl.ds(0, dim)], vec_sem.at[i]) for i, (src, dst) in enumerate(zip(vecs_hbm, vecs))]
    vecs = [v.at[pl.ds(0, dim)] for v in vecs]

    if load_weights:
        def up_copies(i):
            c, w = loads[i]
            return (pltpu.make_async_copy(wg_hbm.at[:, pl.ds(c, w)], wg_v.at[:, pl.ds(c, w)], w_sem.at[0, i]),
                    pltpu.make_async_copy(wu_hbm.at[:, pl.ds(c, w)], wu_v.at[:, pl.ds(c, w)], w_sem.at[1, i]))

        down_copy = pltpu.make_async_copy(wd_hbm, wd_v, d_sem)

        def start_load(i):
            for copy in up_copies(i) if i < len(loads) else [down_copy][i - len(loads):]:
                copy.start()

        start_load(0)
        first = jnp.max(span_ref[0:GROUP // 2, :])
        count = jnp.max(span_ref[GROUP // 2:GROUP, :])
    else:
        note = pltpu.make_async_copy(x_hbm.at[pairs], note_v, note_sem)
        note.start()
        for copy in vec_copies:
            copy.start()
        note.wait()
        first = jnp.max(note_v[0:GROUP // 2, 0:LANES]).astype(jnp.int32)
        count = jnp.max(note_v[GROUP // 2:GROUP, 0:LANES]).astype(jnp.int32)

    n_big = (count + small - 1) // big
    has_small = count > n_big * big

    def start_of(b, size):
        return jnp.minimum(first + b * big, pairs - size)

    def x_copy(b, size):
        where = pl.ds(start_of(b, size), size)
        src = x_hbm.at[where, 0] if load_weights else x_hbm.at[where]
        return pltpu.make_async_copy(src, x_v.at[b, pl.ds(0, size)], x_sem.at[b])

    def x_rows(b, size):
        return x_v[b, pl.ds(0, size)].reshape(size * GROUP, dim).astype(jnp.float32)

    def blocks(items, waits):
        offset = 0
        places = []
        for b, size in items:
            x_copy(b, size).wait()
            mlp_block(size * GROUP, offset, x_rows(b, size), vecs, n_v, u_v, wg_v, wu_v)
            places.append((b, size, offset))
            offset += size * GROUP
        if waits:
            start_load(1)
        for c, w in cols:
            for i, (first_col, _) in enumerate(loads):
                if waits and first_col == c:
                    for copy in up_copies(i):
                        copy.wait()
                    start_load(i + 2)
            for b, size, offset in places:
                up_chunk(size * GROUP, offset, c, w, n_v, u_v, wg_v, wu_v)
        if waits:
            down_copy.wait()
        for b, size, offset in places:
            val = head_value(size * GROUP, offset, x_rows(b, size), vecs, u_v, wd_v)
            base = start_of(b, size)
            for j in range(size):
                at = pl.multiple_of((base + j) * (2 * GROUP) + parity * GROUP, GROUP)
                val_v[pl.ds(at, GROUP), :] = val[j * GROUP:(j + 1) * GROUP]

    for b in range(pairs // big):
        @pl.when(b < n_big)
        def _():
            x_copy(b, big).start()

    @pl.when(has_small)
    def _():
        x_copy(n_big, small).start()

    if load_weights:
        for copy in vec_copies:
            copy.start()

    for copy in vec_copies:
        copy.wait()

    if load_weights:
        @pl.when(n_big >= 2)
        def _():
            blocks([(0, big), (1, big)], True)

        @pl.when(n_big < 2)
        def _():
            for i in range(1, len(loads) + 1):
                start_load(i)
            for i in range(len(loads)):
                for copy in up_copies(i):
                    copy.wait()
            down_copy.wait()

    @pl.loop(jnp.where(n_big >= 2, 2, 0) if load_weights else 0, n_big)
    def _(b):
        blocks([(b, big)], False)

    @pl.when(has_small)
    def _():
        blocks([(n_big, small)], False)

    eye = lax.broadcasted_iota(jnp.int32, (LANES, LANES), 0) == lax.broadcasted_iota(jnp.int32, (LANES, LANES), 1)
    for r in range(out_ref.shape[0]):
        out_ref[r:r + 1, :] = jnp.sum(jnp.where(eye, val_v[r * LANES:(r + 1) * LANES, :], 0.0), axis=0, keepdims=True)


def mlp_call(load_weights, span, seq, vecs, x, weights):
    vmem = pl.BlockSpec(memory_space=pltpu.VMEM)
    hbm = pl.BlockSpec(memory_space=pl.ANY)
    dim, ffn = weights[0].shape
    pairs = seq // (2 * GROUP)
    out_shape = [jax.ShapeDtypeStruct((seq // LANES, LANES), jnp.float32)]
    if load_weights:
        out_shape += [pltpu.VMEM(w.shape, w.dtype) for w in weights]
    max_rows = 2 * BIG if load_weights else BIG
    scratch = [pltpu.VMEM((-(-dim // 1024) * 1024,), jnp.float32)] * 3 + [
        pltpu.VMEM((pairs * GROUP // BIG + 1, BIG // GROUP, GROUP, dim), x.dtype),
        pltpu.VMEM((max_rows, dim), jnp.bfloat16),
        pltpu.VMEM((max_rows, ffn), jnp.bfloat16),
        pltpu.VMEM((seq, LANES), jnp.float32),
        pltpu.SemaphoreType.DMA((3,)),
        pltpu.SemaphoreType.DMA((pairs * GROUP // BIG + 1,)),
    ]
    if load_weights:
        n_loads = len(chunks(ffn, LOAD_COLS))
        scratch += [pltpu.SemaphoreType.DMA((2, n_loads)), pltpu.SemaphoreType.DMA]
    else:
        scratch += [pltpu.VMEM((GROUP, dim), jnp.float32), pltpu.SemaphoreType.DMA]
    tokens = seq // 2
    return pl.pallas_call(
        functools.partial(mlp_kernel, load_weights),
        out_shape=out_shape,
        in_specs=[hbm] * 4 + [vmem] + [hbm] * 3 if load_weights else [hbm] * 4 + [vmem] * 3,
        out_specs=[vmem] * len(out_shape),
        scratch_shapes=scratch,
        compiler_params=pltpu.CompilerParams(vmem_limit_bytes=20 * 1024 * 1024),
        cost_estimate=pl.CostEstimate(flops=6 * tokens * dim * ffn, bytes_accessed=6 * dim * ffn, transcendentals=tokens * ffn),
        name="mlp_own" if load_weights else "mlp_sent",
    )(*[in_hbm(v) for v in vecs], in_hbm(x), *((span, *[in_hbm(w) for w in weights]) if load_weights else weights))


def tail_kernel(dp_size, cp_size, own_ref, sent_ref, rew_ref, mask_ref, bias_ref, val_ref, ret_ref, white_ref, send, recv, back, send_sem, recv_sem, back_sem):
    n_dev = dp_size * cp_size
    n_rows = own_ref.shape[0]
    seq = n_rows * LANES
    me = lax.axis_index('dp') * cp_size + lax.axis_index('cp')
    barrier = pltpu.get_barrier_semaphore()

    def peer(k):
        other = lax.rem(me + k, n_dev)
        return {'dp': other // cp_size, 'cp': lax.rem(other, cp_size)}

    for k in range(1, n_dev):
        pl.semaphore_signal(barrier, inc=1, device_id=peer(k), device_id_type=pl.DeviceIdType.MESH)

    cp = lax.axis_index('cp')
    partner = {'dp': lax.axis_index('dp'), 'cp': cp + 1 - 2 * lax.rem(cp, 2)}
    mask = mask_ref[...].astype(jnp.float32)
    rows = lax.broadcasted_iota(jnp.int32, mask.shape, 0)
    lanes = lax.broadcasted_iota(jnp.int32, mask.shape, 1)
    pos = rows * LANES + lanes
    reward = mask * rew_ref[...]
    row_reach = jnp.exp((LANES - lanes).astype(jnp.float32) * LOG_DECAY)
    reach = jnp.exp((seq - 1 - pos).astype(jnp.float32) * LOG_DECAY)
    m_reach = mask * reach
    fixed = [jnp.sum(a, axis=0, keepdims=True) for a in (mask, m_reach, m_reach * reach)]
    is_own = lax.rem(lanes // GROUP, 2) == 0

    def up_rows(a, k):
        return jnp.where(rows < n_rows - k, pltpu.roll(a, n_rows - k, 0), 0.0)

    pl.semaphore_wait(barrier, n_dev - 1)
    give = pltpu.make_async_remote_copy(
        src_ref=sent_ref, dst_ref=back, send_sem=back_sem.at[0], recv_sem=back_sem.at[1],
        device_id=partner, device_id_type=pl.DeviceIdType.MESH)
    give.start()
    give.wait()
    val = jnp.where(mask > 0, jnp.where(is_own, own_ref[...], back[...]) + bias_ref[...], 0.0)
    val_ref[...] = val

    shifted = pltpu.roll(val, LANES - 1, 1)
    next_val = jnp.where(lanes < LANES - 1, shifted, up_rows(shifted, 1))
    adv = reward + DISCOUNT * next_val - val
    k = 1
    while k < LANES:
        adv = adv + DECAY ** k * jnp.where(lanes < LANES - k, pltpu.roll(adv, LANES - k, 1), 0.0)
        k *= 2
    head = jnp.broadcast_to(adv[:, 0:1], adv.shape)
    k = 1
    while k < n_rows:
        head = head + DECAY ** (LANES * k) * up_rows(head, k)
        k *= 2
    adv = adv + row_reach * up_rows(head, 1)

    m_adv = mask * adv
    at_zero = lanes[0:1] == 0
    moving = [jnp.sum(a, axis=0, keepdims=True) for a in (m_adv, m_adv * adv, m_adv * reach)]
    parts = [fixed[0], moving[0], fixed[1], moving[1], moving[2], fixed[2]]
    parts += [jnp.where(at_zero, val[0:1], 0.0), jnp.where(at_zero, adv[0:1], 0.0)]
    note = jnp.sum(jnp.concatenate(parts, axis=0), axis=1, keepdims=True)
    note = jnp.broadcast_to(note, (8, LANES))
    send[...] = note
    recv[me] = note

    copies = []
    for k in range(1, n_dev):
        copies.append(pltpu.make_async_remote_copy(
            src_ref=send, dst_ref=recv.at[me], send_sem=send_sem.at[k], recv_sem=recv_sem.at[k],
            device_id=peer(k), device_id_type=pl.DeviceIdType.MESH))
    for copy in copies:
        copy.start()
    for copy in copies:
        copy.wait()

    zero = jnp.zeros((1, LANES), jnp.float32)
    count, total, square, mine = zero, zero, zero, zero
    for dp in range(dp_size):
        carry = zero
        for cp in reversed(range(cp_size)):
            q = recv[dp * cp_size + cp]
            count = count + q[0:1]
            total = total + q[1:2] + carry * q[2:3]
            square = square + q[3:4] + carry * (2.0 * q[4:5] + carry * q[5:6])
            mine = jnp.where(me == dp * cp_size + cp, carry, mine)
            carry = DISCOUNT * q[6:7] + DECAY * (q[7:8] + DECAY ** (seq - 1) * carry)
    mean = total / count
    inv = lax.rsqrt(square / count - mean * mean + WHITEN_EPS)
    adv = adv + reach * mine
    ret_ref[...] = adv + val
    white_ref[...] = (adv - mean) * inv


def tail(dp_size, cp_size, own, sent, rew, mask, bias):
    vmem = pl.BlockSpec(memory_space=pltpu.VMEM)
    shape = jax.ShapeDtypeStruct(own.shape, jnp.float32)
    n_dev = dp_size * cp_size
    return pl.pallas_call(
        functools.partial(tail_kernel, dp_size, cp_size),
        out_shape=(shape, shape, shape),
        in_specs=[vmem] * 5,
        out_specs=(vmem, vmem, vmem),
        scratch_shapes=[
            pltpu.VMEM((8, LANES), jnp.float32),
            pltpu.VMEM((n_dev, 8, LANES), jnp.float32),
            pltpu.VMEM(own.shape, jnp.float32),
            pltpu.SemaphoreType.DMA((n_dev,)),
            pltpu.SemaphoreType.DMA((n_dev,)),
            pltpu.SemaphoreType.DMA((2,)),
        ],
        compiler_params=pltpu.CompilerParams(collective_id=0, has_side_effects=True, vmem_limit_bytes=4 * 1024 * 1024),
        name="gae_tail",
    )(own, sent, rew, mask, bias)


def solution(mesh):
    dp_size, cp_size = mesh.shape['dp'], mesh.shape['cp']

    swap = [(i, i ^ 1) for i in range(cp_size)]

    def local_step(x_blk, norm_gain, w_gate, w_up, w_down, final_gain, w_value, b_value, rew_blk, mask_blk):
        shape = rew_blk.shape
        fold = (shape[1] // LANES, LANES)
        mask2 = mask_blk.reshape(fold)
        x4 = x_blk.reshape(shape[1] // (2 * GROUP), 2, GROUP, x_blk.shape[-1])
        vecs = (norm_gain, final_gain, w_value)
        half, span = prep(mask2, x4)
        recv = lax.ppermute(half, 'cp', swap)
        own, *weights = mlp_call(True, span, mask2.size, vecs, x4, (w_gate, w_up, w_down))
        sent, = mlp_call(False, None, mask2.size, vecs, recv, weights)
        val, ret, white = tail(dp_size, cp_size, own, sent, rew_blk.reshape(fold), mask2, b_value.reshape(1, 1))
        mask_f = mask_blk.astype(jnp.float32)
        return mask_f * val.reshape(shape), mask_f * ret.reshape(shape), mask_f * white.reshape(shape)

    tok_spec = P('dp', 'cp')
    in_specs = (P('dp', 'cp', None), P(None), P(None, None), P(None, None), P(None, None), P(None), P(None), P(), tok_spec, tok_spec)
    return jax.shard_map(local_step, mesh=mesh, in_specs=in_specs, out_specs=(tok_spec, tok_spec, tok_spec), check_vma=False)
```

```python
import math
import functools
import jax
import jax.numpy as jnp
from jax import lax
from jax.sharding import PartitionSpec as P
from jax.experimental import pallas as pl
from jax.experimental.pallas import tpu as pltpu

NORM_EPS = 1e-6
WHITEN_EPS = 1e-8
DISCOUNT = 1.0
GAE_LAMBDA = 0.995
LOG_DECAY = math.log(DISCOUNT * GAE_LAMBDA)
DECAY = DISCOUNT * GAE_LAMBDA
LANES = 128
COLS = 256
LOAD_COLS = 1024
GROUP = 16
BIG = 256
SMALL = 128


def chunks(total, step):
    head = total % step
    starts = ([0] if head else []) + list(range(head, total, step))
    return [(start, end - start) for start, end in zip(starts, starts[1:] + [total])]


def in_hbm(x):
    return pltpu.with_memory_space_constraint(x, pltpu.HBM)


def hull(mask, parity):
    rows = lax.broadcasted_iota(jnp.int32, mask.shape, 0)
    lanes = lax.broadcasted_iota(jnp.int32, mask.shape, 1)
    group = rows * (LANES // GROUP) + lanes // GROUP
    live = (mask > 0) & (lax.rem(group, 2) == parity)
    pair = group // 2
    first = jnp.min(jnp.where(live, pair, mask.size))
    last = jnp.max(jnp.where(live, pair, -1))
    return first, jnp.maximum(last - first + 1, 0)


def prep_kernel(mask_hbm, x_hbm, out_hbm, span_ref, mask_v, x_v, out_v, note_v, in_sem, out_sem, mask_sem):
    pairs, _, group, dim = x_hbm.shape
    steps = x_v.shape[0]
    span = pairs // steps

    def load(i):
        body = span - 1 if i == steps - 1 else span
        return pltpu.make_async_copy(x_hbm.at[pl.ds(i * span, body), 1], x_v.at[i, pl.ds(0, body)], in_sem.at[i])

    last_load = pltpu.make_async_copy(x_hbm.at[pairs - 1, 1], x_v.at[steps - 1, span - 1], in_sem.at[steps])

    def store(i):
        return pltpu.make_async_copy(out_v.at[i], out_hbm.at[pl.ds(i * span, span)], out_sem.at[i])

    mask_copy = pltpu.make_async_copy(mask_hbm, mask_v, mask_sem)
    mask_copy.start()
    for i in range(steps):
        load(i).start()
    last_load.start()
    for i in range(steps):
        load(i).wait()
        if i == steps - 1:
            last_load.wait()
        out_v[i] = x_v[i].astype(jnp.float32)
        store(i).start()
    mask_copy.wait()
    first, count = hull(mask_v[...], 1)
    row = lax.broadcasted_iota(jnp.int32, (group, dim), 0)
    note_v[...] = jnp.where(row < group // 2, first, count).astype(jnp.float32)
    note = pltpu.make_async_copy(note_v, out_hbm.at[pairs], out_sem.at[steps])
    note.start()
    first, count = hull(mask_v[...], 0)
    row = lax.broadcasted_iota(jnp.int32, span_ref.shape, 0)
    span_ref[...] = jnp.where(row < group // 2, first, count)
    for i in range(steps):
        store(i).wait()
    note.wait()


def prep(mask2, x4):
    pairs, _, group, dim = x4.shape
    steps = 8
    return pl.pallas_call(
        prep_kernel,
        out_shape=[jax.ShapeDtypeStruct((pairs + 1, group, dim), jnp.float32), pltpu.VMEM((group, LANES), jnp.int32)],
        in_specs=[pl.BlockSpec(memory_space=pl.ANY), pl.BlockSpec(memory_space=pl.ANY)],
        out_specs=[pl.BlockSpec(memory_space=pl.ANY), pl.BlockSpec(memory_space=pltpu.VMEM)],
        scratch_shapes=[
            pltpu.VMEM(mask2.shape, jnp.int32),
            pltpu.VMEM((steps, pairs // steps, group, dim), jnp.bfloat16),
            pltpu.VMEM((steps, pairs // steps, group, dim), jnp.float32),
            pltpu.VMEM((group, dim), jnp.float32),
            pltpu.SemaphoreType.DMA((steps + 1,)),
            pltpu.SemaphoreType.DMA((steps + 1,)),
            pltpu.SemaphoreType.DMA,
        ],
        compiler_params=pltpu.CompilerParams(vmem_limit_bytes=12 * 1024 * 1024),
        name="widen_half",
    )(in_hbm(mask2), in_hbm(x4))


def mlp_block(rows, offset, x_f32, vecs, n_v, u_v, wg_v, wu_v):
    gain_ref = vecs[0]
    dim = x_f32.shape[-1]
    scale = lax.rsqrt(jnp.mean(x_f32 * x_f32, axis=-1, keepdims=True) + NORM_EPS)
    n_v[pl.ds(offset, rows), :] = (x_f32 * scale * gain_ref[...].reshape(1, dim)).astype(jnp.bfloat16)


def up_chunk(rows, offset, c, w, n_v, u_v, wg_v, wu_v):
    n = n_v[pl.ds(offset, rows), :]
    gate = jnp.dot(n, wg_v[:, c:c + w], preferred_element_type=jnp.float32)
    up = jnp.dot(n, wu_v[:, c:c + w], preferred_element_type=jnp.float32)
    u_v[pl.ds(offset, rows), c:c + w] = (jax.nn.silu(gate) * up).astype(jnp.bfloat16)


def head_value(rows, offset, x_f32, vecs, u_v, wd_v):
    _, final_ref, wval_ref = vecs
    dim = x_f32.shape[-1]
    h = x_f32 + jnp.dot(u_v[pl.ds(offset, rows), :], wd_v[...], preferred_element_type=jnp.float32)
    square = jnp.mean(h * h, axis=-1, keepdims=True)
    proj = jnp.sum(h * (final_ref[...] * wval_ref[...]).reshape(1, dim), axis=-1, keepdims=True)
    val = proj * lax.rsqrt(square + NORM_EPS)
    return jnp.broadcast_to(val, (rows, LANES))


def mlp_kernel(load_weights, *refs):
    vecs_hbm, x_hbm, refs = refs[:3], refs[3], refs[4:]
    if load_weights:
        span_ref, wg_hbm, wu_hbm, wd_hbm, out_ref, wg_v, wu_v, wd_v, *refs = refs
        *vecs, x_v, n_v, u_v, val_v, vec_sem, x_sem, w_sem, d_sem = refs
        parity, pairs, dim = 0, x_hbm.shape[0], x_hbm.shape[-1]
    else:
        wg_v, wu_v, wd_v, out_ref, *refs = refs
        *vecs, x_v, n_v, u_v, val_v, vec_sem, x_sem, note_v, note_sem = refs
        parity, pairs, dim = 1, x_hbm.shape[0] - 1, x_hbm.shape[-1]
    ffn = wg_v.shape[1]
    cols = chunks(ffn, COLS)
    loads = chunks(ffn, LOAD_COLS)
    big, small = BIG // GROUP, SMALL // GROUP

    vec_copies = [pltpu.make_async_copy(src, dst.at[pl.ds(0, dim)], vec_sem.at[i]) for i, (src, dst) in enumerate(zip(vecs_hbm, vecs))]
    vecs = [v.at[pl.ds(0, dim)] for v in vecs]

    if load_weights:
        def up_copies(i):
            c, w = loads[i]
            return (pltpu.make_async_copy(wg_hbm.at[:, pl.ds(c, w)], wg_v.at[:, pl.ds(c, w)], w_sem.at[0, i]),
                    pltpu.make_async_copy(wu_hbm.at[:, pl.ds(c, w)], wu_v.at[:, pl.ds(c, w)], w_sem.at[1, i]))

        down_copy = pltpu.make_async_copy(wd_hbm, wd_v, d_sem)

        def start_load(i):
            for copy in up_copies(i) if i < len(loads) else [down_copy][i - len(loads):]:
                copy.start()

        start_load(0)
        first = jnp.max(span_ref[0:GROUP // 2, :])
        count = jnp.max(span_ref[GROUP // 2:GROUP, :])
    else:
        note = pltpu.make_async_copy(x_hbm.at[pairs], note_v, note_sem)
        note.start()
        for copy in vec_copies:
            copy.start()
        note.wait()
        first = jnp.max(note_v[0:GROUP // 2, 0:LANES]).astype(jnp.int32)
        count = jnp.max(note_v[GROUP // 2:GROUP, 0:LANES]).astype(jnp.int32)

    n_big = (count + small - 1) // big
    has_small = count > n_big * big

    def start_of(b, size):
        return jnp.minimum(first + b * big, pairs - size)

    def x_copy(b, size):
        where = pl.ds(start_of(b, size), size)
        src = x_hbm.at[where, 0] if load_weights else x_hbm.at[where]
        return pltpu.make_async_copy(src, x_v.at[b, pl.ds(0, size)], x_sem.at[b])

    def x_rows(b, size):
        return x_v[b, pl.ds(0, size)].reshape(size * GROUP, dim).astype(jnp.float32)

    def blocks(items, waits, first_half=None):
        places = [(b, size, k * BIG) for k, (b, size) in enumerate(items)]

        def gates():
            for b, size, offset in places:
                x_copy(b, size).wait()
                mlp_block(size * GROUP, offset, x_rows(b, size), vecs, n_v, u_v, wg_v, wu_v)
            if waits:
                start_load(1)
            for c, w in cols:
                for i, (first_col, _) in enumerate(loads):
                    if waits and first_col == c:
                        for copy in up_copies(i):
                            copy.wait()
                        start_load(i + 2)
                for b, size, offset in places:
                    up_chunk(size * GROUP, offset, c, w, n_v, u_v, wg_v, wu_v)

        if first_half is None:
            gates()
        else:
            pl.when(first_half)(gates)
        if waits:
            down_copy.wait()
        for b, size, offset in places:
            val = head_value(size * GROUP, offset, x_rows(b, size), vecs, u_v, wd_v)
            base = start_of(b, size)
            for j in range(size):
                at = pl.multiple_of((base + j) * (2 * GROUP) + parity * GROUP, GROUP)
                val_v[pl.ds(at, GROUP), :] = val[j * GROUP:(j + 1) * GROUP]

    for b in range(pairs // big):
        @pl.when(b < n_big)
        def _():
            x_copy(b, big).start()

    @pl.when(has_small)
    def _():
        x_copy(n_big, small).start()

    if load_weights:
        for copy in vec_copies:
            copy.start()

    for copy in vec_copies:
        copy.wait()

    if load_weights:
        @pl.when(n_big >= 2)
        def _():
            blocks([(0, big), (1, big)], True)

        @pl.when(n_big == 0)
        def _():
            for i in range(1, len(loads) + 1):
                start_load(i)
            for i in range(len(loads)):
                for copy in up_copies(i):
                    copy.wait()
            down_copy.wait()

        @pl.when(n_big == 1)
        def _():
            x_copy(0, big).wait()
            mlp_block(BIG, 0, x_rows(0, big), vecs, n_v, u_v, wg_v, wu_v)
            start_load(1)

            @pl.loop(0, ffn // COLS)
            def _(step):
                for i, (first_col, _) in enumerate(loads):
                    @pl.when(step == first_col // COLS)
                    def _():
                        for copy in up_copies(i):
                            copy.wait()
                        start_load(i + 2)

                at = pl.ds(pl.multiple_of(step * COLS, COLS), COLS)
                gate = jnp.dot(n_v[0:BIG, :], wg_v[:, at], preferred_element_type=jnp.float32)
                up = jnp.dot(n_v[0:BIG, :], wu_v[:, at], preferred_element_type=jnp.float32)
                u_v[0:BIG, at] = (jax.nn.silu(gate) * up).astype(jnp.bfloat16)

            down_copy.wait()

    @pl.loop(jnp.where(n_big >= 2, 2, 0) if load_weights else 0, n_big)
    def _(b):
        blocks([(b, big)], False, n_big >= 2 if load_weights else None)

    @pl.when(has_small)
    def _():
        blocks([(n_big, small)], False)

    eye = lax.broadcasted_iota(jnp.int32, (LANES, LANES), 0) == lax.broadcasted_iota(jnp.int32, (LANES, LANES), 1)
    for r in range(out_ref.shape[0]):
        out_ref[r:r + 1, :] = jnp.sum(jnp.where(eye, val_v[r * LANES:(r + 1) * LANES, :], 0.0), axis=0, keepdims=True)


def mlp_call(load_weights, span, seq, vecs, x, weights):
    vmem = pl.BlockSpec(memory_space=pltpu.VMEM)
    hbm = pl.BlockSpec(memory_space=pl.ANY)
    dim, ffn = weights[0].shape
    pairs = seq // (2 * GROUP)
    out_shape = [jax.ShapeDtypeStruct((seq // LANES, LANES), jnp.float32)]
    if load_weights:
        out_shape += [pltpu.VMEM(w.shape, w.dtype) for w in weights]
    max_rows = 2 * BIG if load_weights else BIG
    scratch = [pltpu.VMEM((-(-dim // 1024) * 1024,), jnp.float32)] * 3 + [
        pltpu.VMEM((pairs * GROUP // BIG + 1, BIG // GROUP, GROUP, dim), x.dtype),
        pltpu.VMEM((max_rows, dim), jnp.bfloat16),
        pltpu.VMEM((max_rows, ffn), jnp.bfloat16),
        pltpu.VMEM((seq, LANES), jnp.float32),
        pltpu.SemaphoreType.DMA((3,)),
        pltpu.SemaphoreType.DMA((pairs * GROUP // BIG + 1,)),
    ]
    if load_weights:
        n_loads = len(chunks(ffn, LOAD_COLS))
        scratch += [pltpu.SemaphoreType.DMA((2, n_loads)), pltpu.SemaphoreType.DMA]
    else:
        scratch += [pltpu.VMEM((GROUP, dim), jnp.float32), pltpu.SemaphoreType.DMA]
    tokens = seq // 2
    return pl.pallas_call(
        functools.partial(mlp_kernel, load_weights),
        out_shape=out_shape,
        in_specs=[hbm] * 4 + [vmem] + [hbm] * 3 if load_weights else [hbm] * 4 + [vmem] * 3,
        out_specs=[vmem] * len(out_shape),
        scratch_shapes=scratch,
        compiler_params=pltpu.CompilerParams(vmem_limit_bytes=20 * 1024 * 1024),
        cost_estimate=pl.CostEstimate(flops=6 * tokens * dim * ffn, bytes_accessed=6 * dim * ffn, transcendentals=tokens * ffn),
        name="mlp_own" if load_weights else "mlp_sent",
    )(*[in_hbm(v) for v in vecs], in_hbm(x), *((span, *[in_hbm(w) for w in weights]) if load_weights else weights))


def tail_kernel(dp_size, cp_size, own_ref, sent_ref, rew_ref, mask_ref, bias_ref, val_ref, ret_ref, white_ref, send, recv, back, send_sem, recv_sem, back_sem):
    n_dev = dp_size * cp_size
    n_rows = own_ref.shape[0]
    seq = n_rows * LANES
    me = lax.axis_index('dp') * cp_size + lax.axis_index('cp')
    barrier = pltpu.get_barrier_semaphore()

    def peer(k):
        other = lax.rem(me + k, n_dev)
        return {'dp': other // cp_size, 'cp': lax.rem(other, cp_size)}

    for k in range(1, n_dev):
        pl.semaphore_signal(barrier, inc=1, device_id=peer(k), device_id_type=pl.DeviceIdType.MESH)

    cp = lax.axis_index('cp')
    partner = {'dp': lax.axis_index('dp'), 'cp': cp + 1 - 2 * lax.rem(cp, 2)}
    mask = mask_ref[...].astype(jnp.float32)
    rows = lax.broadcasted_iota(jnp.int32, mask.shape, 0)
    lanes = lax.broadcasted_iota(jnp.int32, mask.shape, 1)
    pos = rows * LANES + lanes
    reward = mask * rew_ref[...]
    row_reach = jnp.exp((LANES - lanes).astype(jnp.float32) * LOG_DECAY)
    reach = jnp.exp((seq - 1 - pos).astype(jnp.float32) * LOG_DECAY)
    m_reach = mask * reach
    fixed = [jnp.sum(a, axis=0, keepdims=True) for a in (mask, m_reach, m_reach * reach)]
    is_own = lax.rem(lanes // GROUP, 2) == 0

    def up_rows(a, k):
        return jnp.where(rows < n_rows - k, pltpu.roll(a, n_rows - k, 0), 0.0)

    pl.semaphore_wait(barrier, n_dev - 1)
    give = pltpu.make_async_remote_copy(
        src_ref=sent_ref, dst_ref=back, send_sem=back_sem.at[0], recv_sem=back_sem.at[1],
        device_id=partner, device_id_type=pl.DeviceIdType.MESH)
    give.start()
    give.wait()
    val = jnp.where(mask > 0, jnp.where(is_own, own_ref[...], back[...]) + bias_ref[...], 0.0)
    val_ref[...] = val

    shifted = pltpu.roll(val, LANES - 1, 1)
    next_val = jnp.where(lanes < LANES - 1, shifted, up_rows(shifted, 1))
    adv = reward + DISCOUNT * next_val - val
    k = 1
    while k < LANES:
        adv = adv + DECAY ** k * jnp.where(lanes < LANES - k, pltpu.roll(adv, LANES - k, 1), 0.0)
        k *= 2
    head = jnp.broadcast_to(adv[:, 0:1], adv.shape)
    k = 1
    while k < n_rows:
        head = head + DECAY ** (LANES * k) * up_rows(head, k)
        k *= 2
    adv = adv + row_reach * up_rows(head, 1)

    m_adv = mask * adv
    at_zero = lanes[0:1] == 0
    moving = [jnp.sum(a, axis=0, keepdims=True) for a in (m_adv, m_adv * adv, m_adv * reach)]
    parts = [fixed[0], moving[0], fixed[1], moving[1], moving[2], fixed[2]]
    parts += [jnp.where(at_zero, val[0:1], 0.0), jnp.where(at_zero, adv[0:1], 0.0)]
    note = jnp.sum(jnp.concatenate(parts, axis=0), axis=1, keepdims=True)
    note = jnp.broadcast_to(note, (8, LANES))
    send[...] = note
    recv[me] = note

    copies = []
    for k in range(1, n_dev):
        copies.append(pltpu.make_async_remote_copy(
            src_ref=send, dst_ref=recv.at[me], send_sem=send_sem.at[k], recv_sem=recv_sem.at[k],
            device_id=peer(k), device_id_type=pl.DeviceIdType.MESH))
    for copy in copies:
        copy.start()
    for copy in copies:
        copy.wait()

    zero = jnp.zeros((1, LANES), jnp.float32)
    count, total, square, mine = zero, zero, zero, zero
    for dp in range(dp_size):
        carry = zero
        for cp in reversed(range(cp_size)):
            q = recv[dp * cp_size + cp]
            count = count + q[0:1]
            total = total + q[1:2] + carry * q[2:3]
            square = square + q[3:4] + carry * (2.0 * q[4:5] + carry * q[5:6])
            mine = jnp.where(me == dp * cp_size + cp, carry, mine)
            carry = DISCOUNT * q[6:7] + DECAY * (q[7:8] + DECAY ** (seq - 1) * carry)
    mean = total / count
    inv = lax.rsqrt(square / count - mean * mean + WHITEN_EPS)
    adv = adv + reach * mine
    ret_ref[...] = adv + val
    white_ref[...] = (adv - mean) * inv


def tail(dp_size, cp_size, own, sent, rew, mask, bias):
    vmem = pl.BlockSpec(memory_space=pltpu.VMEM)
    shape = jax.ShapeDtypeStruct(own.shape, jnp.float32)
    n_dev = dp_size * cp_size
    return pl.pallas_call(
        functools.partial(tail_kernel, dp_size, cp_size),
        out_shape=(shape, shape, shape),
        in_specs=[vmem] * 5,
        out_specs=(vmem, vmem, vmem),
        scratch_shapes=[
            pltpu.VMEM((8, LANES), jnp.float32),
            pltpu.VMEM((n_dev, 8, LANES), jnp.float32),
            pltpu.VMEM(own.shape, jnp.float32),
            pltpu.SemaphoreType.DMA((n_dev,)),
            pltpu.SemaphoreType.DMA((n_dev,)),
            pltpu.SemaphoreType.DMA((2,)),
        ],
        compiler_params=pltpu.CompilerParams(collective_id=0, has_side_effects=True, vmem_limit_bytes=4 * 1024 * 1024),
        name="gae_tail",
    )(own, sent, rew, mask, bias)


def solution(mesh):
    dp_size, cp_size = mesh.shape['dp'], mesh.shape['cp']

    swap = [(i, i ^ 1) for i in range(cp_size)]

    def local_step(x_blk, norm_gain, w_gate, w_up, w_down, final_gain, w_value, b_value, rew_blk, mask_blk):
        shape = rew_blk.shape
        fold = (shape[1] // LANES, LANES)
        mask2 = mask_blk.reshape(fold)
        x4 = x_blk.reshape(shape[1] // (2 * GROUP), 2, GROUP, x_blk.shape[-1])
        vecs = (norm_gain, final_gain, w_value)
        half, span = prep(mask2, x4)
        recv = lax.ppermute(half, 'cp', swap)
        own, *weights = mlp_call(True, span, mask2.size, vecs, x4, (w_gate, w_up, w_down))
        sent, = mlp_call(False, None, mask2.size, vecs, recv, weights)
        val, ret, white = tail(dp_size, cp_size, own, sent, rew_blk.reshape(fold), mask2, b_value.reshape(1, 1))
        mask_f = mask_blk.astype(jnp.float32)
        return mask_f * val.reshape(shape), mask_f * ret.reshape(shape), mask_f * white.reshape(shape)

    tok_spec = P('dp', 'cp')
    in_specs = (P('dp', 'cp', None), P(None), P(None, None), P(None, None), P(None, None), P(None), P(None), P(), tok_spec, tok_spec)
    return jax.shard_map(local_step, mesh=mesh, in_specs=in_specs, out_specs=(tok_spec, tok_spec, tok_spec), check_vma=False)
```
